32 devices in a mesh: dp: 1 (over z), pz: 4 (over y), py: 8 (over x, core).
Axes of the slice: x: 4, y: 4, z: 1, core: 2. Of those that a mesh axis runs over, the one named last changes fastest.
The devices are a block of a 4x4x8 slice.
Arguments:
- rho_re: float32 [24, 128, 128, 128], P('dp', None, 'py', 'pz')
- rho_im: float32 [24, 128, 128, 128], P('dp', None, 'py', 'pz')
- g_re: float32 [128, 128, 128], P('py', 'pz')
- g_im: float32 [128, 128, 128], P('py', 'pz')
Outputs:
- output 1: float32 [24, 128, 128, 128], P('dp', None, 'py', 'pz')
- output 2: float32 [24, 128, 128, 128], P('dp', None, 'py', 'pz')
- output 3: float32 [24, 128, 128, 128], P('dp', 'py', 'pz')
- output 4: float32 [24, 128, 128, 128], P('dp', 'py', 'pz')
All inputs are finite; a program needn't handle non-finite values.
Results may differ from the reference program's by a relative error of at most 0.001.
Values sent between devices are 32-bit elements.
A program may use at most 768 MiB of HBM per device.

```python
import jax
import jax.numpy as jnp
from jax import lax

GRID = 128
FIELDS = 24


def green_kernel():
    positions = jnp.arange(GRID)
    wavenum = jnp.where(positions < (GRID + 1) // 2, positions, positions - GRID).astype(jnp.float32)
    wave_sq = wavenum * wavenum * (16.0 / (GRID * GRID))
    return 1.0 / (1.0 + wave_sq[:, None, None] + 2.0 * wave_sq[None, :, None] + 3.0 * wave_sq[None, None, :])


def setup_inputs(seed: int = 0, part: int = 0) -> dict:
    part_key = jax.random.fold_in(jax.random.key(seed), part)
    key_re, key_im = jax.random.split(part_key)
    field_shape = (FIELDS, GRID, GRID, GRID)
    rho_re = jax.random.normal(key_re, field_shape, jnp.float32)
    rho_im = jax.random.normal(key_im, field_shape, jnp.float32)
    green_re_key, green_im_key = jax.random.split(jax.random.key(seed + 1))
    kernel = green_kernel()
    g_re = kernel * (1.0 + 0.5 * jax.random.normal(green_re_key, kernel.shape, jnp.float32))
    g_im = kernel * (0.5 * jax.random.normal(green_im_key, kernel.shape, jnp.float32))
    return {"rho_re": rho_re, "rho_im": rho_im, "g_re": g_re, "g_im": g_im}


def reference(rho_re, rho_im, g_re, g_im):
    green_fn = lax.complex(g_re, g_im)

    def one_field(field_pair):
        volume = lax.complex(field_pair[0], field_pair[1])
        spectrum = jnp.fft.fftn(volume, axes=(0, 1, 2), norm="ortho") * green_fn
        restored = jnp.fft.ifftn(spectrum, axes=(0, 1, 2), norm="ortho")
        return jnp.real(restored), jnp.imag(restored), jnp.real(spectrum), jnp.imag(spectrum)

    phi_re, phi_im, hat_re, hat_im = lax.map(one_field, (rho_re, rho_im))
    return (phi_re, phi_im, hat_re, hat_im)
```

```python
import functools

import jax
import jax.numpy as jnp
import numpy as np
from jax import lax
from jax.experimental import pallas as pl
from jax.experimental.pallas import tpu as pltpu
from jax.sharding import PartitionSpec as P

MESH = pl.DeviceIdType.MESH
HIGHEST = lax.Precision.HIGHEST


def dft(n, sign):
    angle = 2.0 * np.pi * (np.outer(np.arange(n), np.arange(n)) % n) / n
    cos, sin = np.cos(angle) / np.sqrt(n), sign * np.sin(angle) / np.sqrt(n)
    return np.block([[cos, -sin], [sin, cos]])


def order(n, dims, perm):
    return np.arange(2 * n).reshape((2,) + dims).transpose(perm).reshape(-1)


def swap_blocks(a, lane):
    a = list(a)
    for d, pairs in ((64, ((0, 2), (1, 3))), (32, ((0, 1), (2, 3)))):
        low = (lane // d) % 2 == 0
        for i, j in pairs:
            u, v = a[i], a[j]
            a[i] = jnp.where(low, u, pltpu.roll(v, d, 1))
            a[j] = jnp.where(low, pltpu.roll(u, 128 - d, 1), v)
    return a


def kernel(fields, npy, npz, rho_re, rho_im, g_re, g_im, w1, w2, w3, w4, w5, w6,
           phi_re, phi_im, hat_re, hat_im,
           rho, hat, phi, work, send1, send2, send3, send4, recv1, recv2, recv3, recv4,
           in_sem, hat_sem, phi_sem, send_sem, recv_sem):
    py, pz = lax.axis_index("py"), lax.axis_index("pz")
    xrows, yrows = recv1.shape[1] // npy, recv2.shape[1] // npz
    lane = lax.broadcasted_iota(jnp.int32, (32, 128), 1)

    barrier = pltpu.get_barrier_semaphore()
    for j in range(1, npy):
        pl.semaphore_signal(barrier, inc=1, device_id={"py": lax.rem(py + j, npy)}, device_id_type=MESH)
    for j in range(1, npz):
        pl.semaphore_signal(barrier, inc=1, device_id={"pz": lax.rem(pz + j, npz)}, device_id_type=MESH)
    pl.semaphore_wait(barrier, npy + npz - 2)

    def load(f, slot):
        return [pltpu.make_async_copy(src.at[f], rho.at[slot, c], in_sem.at[slot, c])
                for c, src in enumerate((rho_re, rho_im))]

    def store(dsts, buf, sem, f, slot):
        return [pltpu.make_async_copy(buf.at[slot, c], dst.at[f], sem.at[slot, c]) for c, dst in enumerate(dsts)]

    def exchange(stage, axis, send, recv, f, slot):
        me, n, rows = (py, npy, xrows) if axis == "py" else (pz, npz, yrows)
        mine = pl.ds(pl.multiple_of(me * rows, rows), rows)
        for j in range(1, n):
            to = lax.rem(me + j, n)
            pltpu.make_async_remote_copy(
                src_ref=send.at[slot, pl.ds(pl.multiple_of(to * rows, rows), rows), :], dst_ref=recv.at[f, mine, :],
                send_sem=send_sem.at[stage, slot], recv_sem=recv_sem.at[stage, f],
                device_id={axis: to}, device_id_type=MESH).start()
        pltpu.make_async_copy(send.at[slot, mine, :], recv.at[f, mine, :], recv_sem.at[stage, f]).start()

    def wait_sent(stage, send, slot, rows):
        part = send.at[slot, pl.ds(0, send.shape[1] - rows), :]
        pltpu.make_async_copy(part, part, send_sem.at[stage, slot]).wait()

    def wait_received(stage, recv, f):
        pltpu.make_async_copy(recv.at[f], recv.at[f], recv_sem.at[stage, f]).wait()

    for cp in load(0, 0):
        cp.start()

    def step(s, carry):
        @pl.when(s < fields)
        def _():
            f, slot = s, lax.rem(s, 2)

            @pl.when(f + 1 < fields)
            def _():
                for cp in load(f + 1, 1 - slot):
                    cp.start()
            for cp in load(f, slot):
                cp.wait()

            @pl.when(f >= 2)
            def _():
                wait_sent(0, send1, slot, xrows)
            volume = jnp.concatenate([rho[slot, 0], rho[slot, 1]], axis=1)
            out = lax.dot_general(w1[...], volume, (((1,), (1,)), ((), ())), precision=HIGHEST,
                                  preferred_element_type=jnp.float32)
            for p in range(8):
                for t in range(4):
                    send1[slot, p * 128 + t * 32:p * 128 + (t + 1) * 32, :] = out[p * 32:(p + 1) * 32, t * 128:(t + 1) * 128]
            exchange(0, "py", send1, recv1, f, slot)

        @pl.when((s >= 1) & (s < fields + 1))
        def _():
            f = s - 1
            slot = lax.rem(f, 2)
            wait_received(0, recv1, f)
            for c in range(2):
                for g in range(4):
                    blocks = [recv1[f, pl.ds(c * 16 + 4 * g + k, 32, stride=32), :] for k in range(4)]
                    for y, b in enumerate(swap_blocks(blocks, lane)):
                        work[c * 128 + y * 32:c * 128 + (y + 1) * 32, g * 128:(g + 1) * 128] = b

            @pl.when(f >= 2)
            def _():
                wait_sent(1, send2, slot, yrows)
            send2[slot] = jnp.dot(w2[...], work[...], precision=HIGHEST, preferred_element_type=jnp.float32)
            exchange(1, "pz", send2, recv2, f, slot)

        @pl.when((s >= 2) & (s < fields + 2))
        def _():
            f = s - 2
            slot = lax.rem(f, 2)
            wait_received(1, recv2, f)
            cols = []
            for c in range(2):
                rows = []
                for g in range(4):
                    blocks = [recv2[f, b * 64 + c * 32:b * 64 + (c + 1) * 32, g * 128:(g + 1) * 128] for b in range(4)]
                    rows += swap_blocks(blocks, lane)
                cols.append(jnp.concatenate(rows, axis=0))
            spec = jnp.dot(jnp.concatenate(cols, axis=1), w3[...], precision=HIGHEST, preferred_element_type=jnp.float32)
            sr, si = spec[:, :128], spec[:, 128:]

            @pl.when(f >= 2)
            def _():
                for cp in store((hat_re, hat_im), hat, hat_sem, f, slot):
                    cp.wait()
                wait_sent(2, send3, slot, yrows)
            hat[slot, 0] = sr * g_re[...] - si * g_im[...]
            hat[slot, 1] = sr * g_im[...] + si * g_re[...]
            for cp in store((hat_re, hat_im), hat, hat_sem, f, slot):
                cp.start()
            back = jnp.dot(jnp.concatenate([hat[slot, 0], hat[slot, 1]], axis=1), w4[...], precision=HIGHEST,
                           preferred_element_type=jnp.float32)
            for c in range(2):
                for g in range(4):
                    blocks = [back[(4 * g + k) * 32:(4 * g + k + 1) * 32, c * 128:(c + 1) * 128] for k in range(4)]
                    for b, block in enumerate(swap_blocks(blocks, lane)):
                        send3[slot, b * 64 + c * 32:b * 64 + (c + 1) * 32, g * 128:(g + 1) * 128] = block
            exchange(2, "pz", send3, recv3, f, slot)

        @pl.when((s >= 3) & (s < fields + 3))
        def _():
            f = s - 3
            slot = lax.rem(f, 2)
            wait_received(2, recv3, f)

            @pl.when(f >= 2)
            def _():
                wait_sent(3, send4, slot, xrows)
            back = jnp.dot(w5[...], recv3[f], precision=HIGHEST, preferred_element_type=jnp.float32)
            for c in range(2):
                for g in range(4):
                    blocks = [back[c * 128 + y * 32:c * 128 + (y + 1) * 32, g * 128:(g + 1) * 128] for y in range(4)]
                    for k, block in enumerate(swap_blocks(blocks, lane)):
                        send4[slot, pl.ds(c * 16 + 4 * g + k, 32, stride=32), :] = block
            exchange(3, "py", send4, recv4, f, slot)

        @pl.when(s >= 4)
        def _():
            f = s - 4
            slot = lax.rem(f, 2)
            wait_received(3, recv4, f)

            @pl.when(f >= 2)
            def _():
                for cp in store((phi_re, phi_im), phi, phi_sem, f, slot):
                    cp.wait()
            lines = []
            for t in range(4):
                block = jnp.concatenate([recv4[f, p * 128 + t * 32:p * 128 + (t + 1) * 32, :] for p in range(8)], axis=0)
                lines.append(block.T)
            out = jnp.dot(jnp.concatenate(lines, axis=0), w6[...], precision=HIGHEST, preferred_element_type=jnp.float32)
            phi[slot, 0] = out[:, :128]
            phi[slot, 1] = out[:, 128:]
            for cp in store((phi_re, phi_im), phi, phi_sem, f, slot):
                cp.start()

        return carry

    lax.fori_loop(0, fields + 4, step, 0)
    for slot in range(2):
        for cp in store((hat_re, hat_im), hat, hat_sem, 0, slot) + store((phi_re, phi_im), phi, phi_sem, 0, slot):
            cp.wait()
        wait_sent(0, send1, slot, xrows)
        wait_sent(1, send2, slot, yrows)
        wait_sent(2, send3, slot, yrows)
        wait_sent(3, send4, slot, xrows)


def solution(mesh):
    npy, npz = mesh.shape["py"], mesh.shape["pz"]

    def local_solve(rho_re, rho_im, g_re, g_im):
        fields, n, ny, nz = rho_re.shape
        kx, ky = n // npy, n // npz
        fwd, inv = dft(n, -1), dft(n, 1)
        natural = np.arange(2 * n)
        x_blocks = order(n, (npy, kx), (1, 0, 2))
        y_blocks = order(n, (npz, ky), (1, 0, 2))
        y_mixed = order(n, (npy, ny // 4, 4), (0, 3, 1, 2))
        pick = lambda m, r, c: jnp.asarray(m[np.ix_(r, c)].astype(np.float32))
        mats = (pick(fwd, x_blocks, natural), pick(fwd, y_blocks, y_mixed), pick(fwd, natural, natural).T,
                pick(inv, natural, natural).T, pick(inv, y_mixed, y_blocks), pick(inv, natural, x_blocks).T)
        lines = ny * nz
        space = lambda v: v.transpose(0, 2, 3, 1).reshape(fields, lines, n)
        sent = 2 * lines
        f32 = jnp.float32
        out = pl.pallas_call(
            functools.partial(kernel, fields, npy, npz),
            out_shape=[jax.ShapeDtypeStruct((fields, lines, n), f32)] * 4,
            in_specs=[pl.BlockSpec(memory_space=pl.ANY)] * 2 + [pl.BlockSpec(memory_space=pltpu.VMEM)] * 8,
            out_specs=[pl.BlockSpec(memory_space=pl.ANY)] * 4,
            scratch_shapes=[
                pltpu.VMEM((2, 2, lines, n), f32), pltpu.VMEM((2, 2, lines, n), f32), pltpu.VMEM((2, 2, lines, n), f32),
                pltpu.VMEM((2 * n, lines), f32),
                pltpu.VMEM((2, sent, n), f32), pltpu.VMEM((2, 2 * n, lines), f32),
                pltpu.VMEM((2, 2 * n, lines), f32), pltpu.VMEM((2, sent, n), f32),
                pltpu.VMEM((fields, sent, n), f32), pltpu.VMEM((fields, 2 * n, lines), f32),
                pltpu.VMEM((fields, 2 * n, lines), f32), pltpu.VMEM((fields, sent, n), f32),
                pltpu.SemaphoreType.DMA((2, 2)), pltpu.SemaphoreType.DMA((2, 2)), pltpu.SemaphoreType.DMA((2, 2)),
                pltpu.SemaphoreType.DMA((4, 2)), pltpu.SemaphoreType.DMA((4, fields)),
            ],
            compiler_params=pltpu.CompilerParams(collective_id=0, has_side_effects=True, vmem_limit_bytes=67043328),
        )(space(rho_re), space(rho_im), g_re.reshape(lines, n), g_im.reshape(lines, n), *mats)
        grid = lambda v: v.reshape(fields, ny, nz, n).transpose(0, 3, 1, 2)
        wave = lambda v: v.reshape(fields, kx, ky, n)
        return grid(out[0]), grid(out[1]), wave(out[2]), wave(out[3])

    space_layout = P("dp", None, "py", "pz")
    wave_layout = P("dp", "py", "pz", None)
    green_layout = P("py", "pz", None)
    return jax.shard_map(local_solve, mesh=mesh,
                         in_specs=(space_layout, space_layout, green_layout, green_layout),
                         out_specs=(space_layout, space_layout, wave_layout, wave_layout),
                         check_vma=False)
```

```python
import functools

import jax
import jax.numpy as jnp
import numpy as np
from jax import lax
from jax.experimental import pallas as pl
from jax.experimental.pallas import tpu as pltpu
from jax.sharding import PartitionSpec as P

MESH = pl.DeviceIdType.MESH
HIGHEST = lax.Precision.HIGHEST
RING = 8
SLOTS = 4


def dft(n, sign):
    angle = 2.0 * np.pi * (np.outer(np.arange(n), np.arange(n)) % n) / n
    cos, sin = np.cos(angle) / np.sqrt(n), sign * np.sin(angle) / np.sqrt(n)
    return np.block([[cos, -sin], [sin, cos]])


def order(n, dims, perm):
    return np.arange(2 * n).reshape((2,) + dims).transpose(perm).reshape(-1)


def swap_blocks(a, lane):
    a = list(a)
    for d, pairs in ((64, ((0, 2), (1, 3))), (32, ((0, 1), (2, 3)))):
        low = (lane // d) % 2 == 0
        for i, j in pairs:
            u, v = a[i], a[j]
            a[i] = jnp.where(low, u, pltpu.roll(v, d, 1))
            a[j] = jnp.where(low, pltpu.roll(u, 128 - d, 1), v)
    return a


def kernel(fields, npy, npz, rho_re, rho_im, green_re, green_im, m1, m2, m3, m4, m5, m6,
           phi_re, phi_im, hat_re, hat_im,
           g_re, g_im, w1, w2, w3, w4, w5, w6, rho, hat, phi, work,
           send1, send2, send3, send4, recv1, recv2, recv3, recv4,
           const_sem, in_sem, hat_sem, phi_sem, send_sem, recv_sem):
    py, pz = lax.axis_index("py"), lax.axis_index("pz")
    chunks = 2 * fields
    lane = lax.broadcasted_iota(jnp.int32, (32, 128), 1)

    def load(f, slot):
        return [pltpu.make_async_copy(src.at[f], rho.at[slot, c], in_sem.at[slot, c])
                for c, src in enumerate((rho_re, rho_im))]

    def store(dsts, buf, sem, i, slot):
        return [pltpu.make_async_copy(buf.at[slot, c], dst.at[i], sem.at[slot, c]) for c, dst in enumerate(dsts)]

    consts = [pltpu.make_async_copy(src, dst, const_sem.at[i]) for i, (src, dst) in enumerate(zip(
        (m1, m2, m3, m4, m5, m6, green_re, green_im), (w1, w2, w3, w4, w5, w6, g_re, g_im)))]
    for cp in load(0, 0) + consts:
        cp.start()

    barrier = pltpu.get_barrier_semaphore()
    for j in range(1, npy):
        pl.semaphore_signal(barrier, inc=1, device_id={"py": lax.rem(py + j, npy)}, device_id_type=MESH)
    for j in range(1, npz):
        pl.semaphore_signal(barrier, inc=1, device_id={"pz": lax.rem(pz + j, npz)}, device_id_type=MESH)
    pl.semaphore_wait(barrier, npy + npz - 2)
    for cp in consts:
        cp.wait()

    def exchange(stage, axis, send, recv, c):
        me, n = (py, npy) if axis == "py" else (pz, npz)
        rows = recv.shape[1] // n
        slot, ring = lax.rem(c, SLOTS), lax.rem(c, RING)
        mine = pl.ds(pl.multiple_of(me * rows, rows), rows)
        for j in range(1, n):
            to = lax.rem(me + j, n)
            pltpu.make_async_remote_copy(
                src_ref=send.at[slot, pl.ds(pl.multiple_of(to * rows, rows), rows), :], dst_ref=recv.at[ring, mine, :],
                send_sem=send_sem.at[stage, slot], recv_sem=recv_sem.at[stage, ring],
                device_id={axis: to}, device_id_type=MESH).start()
        pltpu.make_async_copy(send.at[slot, mine, :], recv.at[ring, mine, :], recv_sem.at[stage, ring]).start()

    def wait_sent(stage, axis, send, slot):
        n = npy if axis == "py" else npz
        part = send.at[slot, pl.ds(0, send.shape[1] // n * (n - 1)), :]
        pltpu.make_async_copy(part, part, send_sem.at[stage, slot]).wait()

    def wait_received(stage, recv, c):
        ring = lax.rem(c, RING)
        pltpu.make_async_copy(recv.at[ring], recv.at[ring], recv_sem.at[stage, ring]).wait()

    def step(u, carry):
        @pl.when((lax.rem(u, 2) == 0) & (u < chunks))
        def _():
            f = lax.div(u, 2)
            slot = lax.rem(f, 2)

            @pl.when(f + 1 < fields)
            def _():
                for cp in load(f + 1, 1 - slot):
                    cp.start()
            for cp in load(f, slot):
                cp.wait()
            volume = jnp.concatenate([rho[slot, 0], rho[slot, 1]], axis=1)
            for h in range(2):
                c = u + h
                to = lax.rem(c, SLOTS)

                @pl.when(c >= SLOTS)
                def _():
                    wait_sent(0, "py", send1, to)
                out = lax.dot_general(w1[h * 128:(h + 1) * 128, :], volume, (((1,), (1,)), ((), ())), precision=HIGHEST,
                                      preferred_element_type=jnp.float32)
                for p in range(8):
                    for t in range(4):
                        send1[to, p * 64 + t * 16:p * 64 + (t + 1) * 16, :] = out[p * 16:(p + 1) * 16, t * 128:(t + 1) * 128]
                exchange(0, "py", send1, recv1, c)

        @pl.when((u >= 2) & (u < chunks + 2))
        def _():
            c = u - 2
            to, ring = lax.rem(c, SLOTS), lax.rem(c, RING)
            wait_received(0, recv1, c)
            for part in range(2):
                for g in range(2):
                    blocks = [recv1[ring, pl.ds(part * 8 + 4 * g + k, 32, stride=16), :] for k in range(4)]
                    for y, b in enumerate(swap_blocks(blocks, lane)):
                        work[part * 128 + y * 32:part * 128 + (y + 1) * 32, g * 128:(g + 1) * 128] = b

            @pl.when(c >= SLOTS)
            def _():
                wait_sent(1, "pz", send2, to)
            send2[to] = jnp.dot(w2[...], work[...], precision=HIGHEST, preferred_element_type=jnp.float32)
            exchange(1, "pz", send2, recv2, c)

        @pl.when((u >= 4) & (u < chunks + 4))
        def _():
            c = u - 4
            to, ring, slot = lax.rem(c, SLOTS), lax.rem(c, RING), lax.rem(c, 2)
            wait_received(1, recv2, c)
            cols = []
            for part in range(2):
                rows = []
                for g in range(2):
                    blocks = [recv2[ring, b * 64 + part * 32:b * 64 + (part + 1) * 32, g * 128:(g + 1) * 128]
                              for b in range(4)]
                    rows += swap_blocks(blocks, lane)
                cols.append(jnp.concatenate(rows, axis=0))
            spec = jnp.dot(jnp.concatenate(cols, axis=1), w3[...], precision=HIGHEST, preferred_element_type=jnp.float32)
            sr, si = spec[:, :128], spec[:, 128:]

            @pl.when(c >= 2)
            def _():
                for cp in store((hat_re, hat_im), hat, hat_sem, c, slot):
                    cp.wait()

            @pl.when(c >= SLOTS)
            def _():
                wait_sent(2, "pz", send3, to)
            gr, gi = g_re[slot], g_im[slot]
            hat[slot, 0] = sr * gr - si * gi
            hat[slot, 1] = sr * gi + si * gr
            for cp in store((hat_re, hat_im), hat, hat_sem, c, slot):
                cp.start()
            back = jnp.dot(jnp.concatenate([hat[slot, 0], hat[slot, 1]], axis=1), w4[...], precision=HIGHEST,
                           preferred_element_type=jnp.float32)
            for part in range(2):
                for g in range(2):
                    blocks = [back[(4 * g + k) * 32:(4 * g + k + 1) * 32, part * 128:(part + 1) * 128] for k in range(4)]
                    for b, block in enumerate(swap_blocks(blocks, lane)):
                        send3[to, b * 64 + part * 32:b * 64 + (part + 1) * 32, g * 128:(g + 1) * 128] = block
            exchange(2, "pz", send3, recv3, c)

        @pl.when((u >= 6) & (u < chunks + 6))
        def _():
            c = u - 6
            to, ring = lax.rem(c, SLOTS), lax.rem(c, RING)
            wait_received(2, recv3, c)

            @pl.when(c >= SLOTS)
            def _():
                wait_sent(3, "py", send4, to)
            back = jnp.dot(w5[...], recv3[ring], precision=HIGHEST, preferred_element_type=jnp.float32)
            for part in range(2):
                for g in range(2):
                    blocks = [back[part * 128 + y * 32:part * 128 + (y + 1) * 32, g * 128:(g + 1) * 128] for y in range(4)]
                    for k, block in enumerate(swap_blocks(blocks, lane)):
                        send4[to, pl.ds(part * 8 + 4 * g + k, 32, stride=16), :] = block
            exchange(3, "py", send4, recv4, c)

        @pl.when((lax.rem(u, 2) == 0) & (u >= 8))
        def _():
            c = u - 8
            f = lax.div(c, 2)
            slot = lax.rem(f, 2)
            for h in range(2):
                wait_received(3, recv4, c + h)

            @pl.when(f >= 2)
            def _():
                for cp in store((phi_re, phi_im), phi, phi_sem, f, slot):
                    cp.wait()
            lines = []
            for t in range(4):
                block = jnp.concatenate([recv4[lax.rem(c + h, RING), p * 64 + t * 16:p * 64 + (t + 1) * 16, :]
                                         for h in range(2) for p in range(8)], axis=0)
                lines.append(block.T)
            out = jnp.dot(jnp.concatenate(lines, axis=0), w6[...], precision=HIGHEST, preferred_element_type=jnp.float32)
            phi[slot, 0] = out[:, :128]
            phi[slot, 1] = out[:, 128:]
            for cp in store((phi_re, phi_im), phi, phi_sem, f, slot):
                cp.start()

        return carry

    lax.fori_loop(0, chunks + 7, step, 0)
    for slot in range(2):
        for cp in store((hat_re, hat_im), hat, hat_sem, 0, slot) + store((phi_re, phi_im), phi, phi_sem, 0, slot):
            cp.wait()
    for slot in range(SLOTS):
        wait_sent(0, "py", send1, slot)
        wait_sent(1, "pz", send2, slot)
        wait_sent(2, "pz", send3, slot)
        wait_sent(3, "py", send4, slot)


def write_out(*refs):
    n = len(refs) // 2
    copies = [pltpu.make_async_copy(refs[i], refs[n + i], refs[-1].at[i]) for i in range(n)]
    for cp in copies:
        cp.start()
    for cp in copies:
        cp.wait()


def solution(mesh):
    npy, npz = mesh.shape["py"], mesh.shape["pz"]

    def local_solve(rho_re, rho_im, g_re, g_im):
        fields, n, ny, nz = rho_re.shape
        kx, ky = n // npy, n // npz
        fwd, inv = dft(n, -1), dft(n, 1)
        natural = np.arange(2 * n)
        x_blocks = order(n, (npy, 2, kx // 2), (2, 1, 0, 3))
        y_blocks = order(n, (npz, ky), (1, 0, 2))
        y_mixed = order(n, (npy, ny // 4, 4), (0, 3, 1, 2))
        pick = lambda m, r, c: jnp.asarray(m[np.ix_(r, c)].astype(np.float32))
        mats = (pick(fwd, x_blocks, natural), pick(fwd, y_blocks, y_mixed), pick(fwd.T, natural, natural),
                pick(inv.T, natural, natural), pick(inv, y_mixed, y_blocks), pick(inv.T, x_blocks, natural))
        lines = ny * nz
        half = lines // 2
        f32, any_space = jnp.float32, pl.BlockSpec(memory_space=pl.ANY)
        space = lambda v: v.transpose(0, 2, 3, 1).reshape(fields, lines, n)
        held = ((fields, lines, n),) * 2 + ((2 * fields, half, n),) * 2
        x_buf, y_buf = (lines, n), (2 * n, 2 * n)
        out = pl.pallas_call(
            functools.partial(kernel, fields, npy, npz),
            out_shape=[pltpu.VMEM(s, f32) for s in held],
            in_specs=[any_space] * 10,
            out_specs=[any_space] * 4,
            scratch_shapes=[pltpu.VMEM((2, half, n), f32)] * 2 + [pltpu.VMEM((2 * n, 2 * n), f32)] * 6 + [
                pltpu.VMEM((2, 2, lines, n), f32), pltpu.VMEM((2, 2, half, n), f32), pltpu.VMEM((2, 2, lines, n), f32),
                pltpu.VMEM(y_buf, f32)] + [
                pltpu.VMEM((SLOTS,) + b, f32) for b in (x_buf, y_buf, y_buf, x_buf)] + [
                pltpu.VMEM((RING,) + b, f32) for b in (x_buf, y_buf, y_buf, x_buf)] + [
                pltpu.SemaphoreType.DMA((8,)),
                pltpu.SemaphoreType.DMA((2, 2)), pltpu.SemaphoreType.DMA((2, 2)), pltpu.SemaphoreType.DMA((2, 2)),
                pltpu.SemaphoreType.DMA((4, SLOTS)), pltpu.SemaphoreType.DMA((4, RING)),
            ],
            compiler_params=pltpu.CompilerParams(collective_id=0, has_side_effects=True, vmem_limit_bytes=34 * 2**20),
        )(space(rho_re), space(rho_im), g_re.reshape(2, half, n), g_im.reshape(2, half, n), *mats)
        out = pl.pallas_call(
            write_out,
            out_shape=[jax.ShapeDtypeStruct(s, f32) for s in held],
            in_specs=[any_space] * 4, out_specs=[any_space] * 4,
            scratch_shapes=[pltpu.SemaphoreType.DMA((4,))],
            compiler_params=pltpu.CompilerParams(vmem_limit_bytes=2**20),
        )(*[pltpu.with_memory_space_constraint(v, pltpu.VMEM) for v in out])
        grid = lambda v: v.reshape(fields, ny, nz, n).transpose(0, 3, 1, 2)
        wave = lambda v: v.reshape(fields, kx, ky, n)
        return grid(out[0]), grid(out[1]), wave(out[2]), wave(out[3])

    space_layout = P("dp", None, "py", "pz")
    wave_layout = P("dp", "py", "pz", None)
    green_layout = P("py", "pz", None)
    return jax.shard_map(local_solve, mesh=mesh,
                         in_specs=(space_layout, space_layout, green_layout, green_layout),
                         out_specs=(space_layout, space_layout, wave_layout, wave_layout),
                         check_vma=False)
```

```python
import functools

import jax
import jax.numpy as jnp
import numpy as np
from jax import lax
from jax.experimental import pallas as pl
from jax.experimental.pallas import tpu as pltpu
from jax.sharding import PartitionSpec as P

MESH = pl.DeviceIdType.MESH
HIGHEST = lax.Precision.HIGHEST
RING = 8
SLOTS = 4


def dft(n, sign):
    angle = 2.0 * np.pi * (np.outer(np.arange(n), np.arange(n)) % n) / n
    cos, sin = np.cos(angle) / np.sqrt(n), sign * np.sin(angle) / np.sqrt(n)
    return np.block([[cos, -sin], [sin, cos]])


def order(n, dims, perm):
    return np.arange(2 * n).reshape((2,) + dims).transpose(perm).reshape(-1)


def swap_blocks(a, lane):
    a = list(a)
    for d, pairs in ((64, ((0, 2), (1, 3))), (32, ((0, 1), (2, 3)))):
        low = (lane // d) % 2 == 0
        for i, j in pairs:
            u, v = a[i], a[j]
            a[i] = jnp.where(low, u, pltpu.roll(v, d, 1))
            a[j] = jnp.where(low, pltpu.roll(u, 128 - d, 1), v)
    return a


def last_dft(chunk, w):
    lines = []
    for t in range(4):
        block = jnp.concatenate([chunk(h, slice(p * 64 + t * 16, p * 64 + (t + 1) * 16)) for h in range(2) for p in range(8)],
                                axis=0)
        lines.append(block.T)
    return jnp.dot(jnp.concatenate(lines, axis=0), w[...], precision=HIGHEST, preferred_element_type=jnp.float32)


def kernel(fields, npy, npz, rho_re, rho_im, green_re, green_im, m1, m2, m3, m4, m5, m6,
           phi_re, phi_im, hat_re, hat_im, recv4,
           g_re, g_im, w1, w2, w3, w4, w5, w6, rho, work,
           send1, send2, send3, send4, recv1, recv2, recv3,
           const_sem, in_sem, send_sem, recv_sem):
    py, pz = lax.axis_index("py"), lax.axis_index("pz")
    chunks = 2 * fields
    lane = lax.broadcasted_iota(jnp.int32, (32, 128), 1)

    def load(f, slot):
        return [pltpu.make_async_copy(src.at[f], rho.at[slot, c], in_sem.at[slot, c])
                for c, src in enumerate((rho_re, rho_im))]

    consts = [pltpu.make_async_copy(src, dst, const_sem.at[i]) for i, (src, dst) in enumerate(zip(
        (m1, m2, m3, m4, m5, m6, green_re, green_im), (w1, w2, w3, w4, w5, w6, g_re, g_im)))]
    for cp in load(0, 0) + consts:
        cp.start()

    barrier = pltpu.get_barrier_semaphore()
    for j in range(1, npy):
        pl.semaphore_signal(barrier, inc=1, device_id={"py": lax.rem(py + j, npy)}, device_id_type=MESH)
    for j in range(1, npz):
        pl.semaphore_signal(barrier, inc=1, device_id={"pz": lax.rem(pz + j, npz)}, device_id_type=MESH)
    consts[0].wait()

    def exchange(stage, axis, send, recv, c):
        me, n = (py, npy) if axis == "py" else (pz, npz)
        rows = recv.shape[1] // n
        slot, ring = lax.rem(c, SLOTS), lax.rem(c, RING)
        mine = pl.ds(pl.multiple_of(me * rows, rows), rows)
        for j in sorted(range(1, n), key=lambda j: -min(j, n - j)):
            to = lax.rem(me + j, n)
            pltpu.make_async_remote_copy(
                src_ref=send.at[slot, pl.ds(pl.multiple_of(to * rows, rows), rows), :], dst_ref=recv.at[ring, mine, :],
                send_sem=send_sem.at[stage, slot], recv_sem=recv_sem.at[stage, ring],
                device_id={axis: to}, device_id_type=MESH).start()
        pltpu.make_async_copy(send.at[slot, mine, :], recv.at[ring, mine, :], recv_sem.at[stage, ring]).start()

    def wait_sent(stage, axis, send, slot):
        n = npy if axis == "py" else npz
        part = send.at[slot, pl.ds(0, send.shape[1] // n * (n - 1)), :]
        pltpu.make_async_copy(part, part, send_sem.at[stage, slot]).wait()

    def wait_received(stage, recv, c):
        ring = lax.rem(c, RING)
        pltpu.make_async_copy(recv.at[ring], recv.at[ring], recv_sem.at[stage, ring]).wait()

    def step(u, carry):
        @pl.when((lax.rem(u, 2) == 0) & (u < chunks))
        def _():
            f = lax.div(u, 2)
            slot = lax.rem(f, 2)

            @pl.when(f + 1 < fields)
            def _():
                for cp in load(f + 1, 1 - slot):
                    cp.start()
            for cp in load(f, slot):
                cp.wait()
            volume = jnp.concatenate([rho[slot, 0], rho[slot, 1]], axis=1)
            for h in range(2):
                c = u + h
                to = lax.rem(c, SLOTS)

                @pl.when(c >= SLOTS)
                def _():
                    wait_sent(0, "py", send1, to)
                out = lax.dot_general(w1[h * 128:(h + 1) * 128, :], volume, (((1,), (1,)), ((), ())), precision=HIGHEST,
                                      preferred_element_type=jnp.float32)
                if h == 0:
                    @pl.when(u == 0)
                    def _():
                        pl.semaphore_wait(barrier, npy + npz - 2)
                        for cp in consts[1:]:
                            cp.wait()
                for p in range(8):
                    for t in range(4):
                        send1[to, p * 64 + t * 16:p * 64 + (t + 1) * 16, :] = out[p * 16:(p + 1) * 16, t * 128:(t + 1) * 128]
                exchange(0, "py", send1, recv1, c)

        @pl.when((u >= 2) & (u < chunks + 2))
        def _():
            c = u - 2
            to, ring = lax.rem(c, SLOTS), lax.rem(c, RING)
            wait_received(0, recv1, c)
            for part in range(2):
                for g in range(2):
                    blocks = [recv1[ring, pl.ds(part * 8 + 4 * g + k, 32, stride=16), :] for k in range(4)]
                    for y, b in enumerate(swap_blocks(blocks, lane)):
                        work[part * 128 + y * 32:part * 128 + (y + 1) * 32, g * 128:(g + 1) * 128] = b

            @pl.when(c >= SLOTS)
            def _():
                wait_sent(1, "pz", send2, to)
            send2[to] = jnp.dot(w2[...], work[...], precision=HIGHEST, preferred_element_type=jnp.float32)
            exchange(1, "pz", send2, recv2, c)

        @pl.when((u >= 4) & (u < chunks + 4))
        def _():
            c = u - 4
            to, ring, slot = lax.rem(c, SLOTS), lax.rem(c, RING), lax.rem(c, 2)
            wait_received(1, recv2, c)
            cols = []
            for part in range(2):
                rows = []
                for g in range(2):
                    blocks = [recv2[ring, b * 64 + part * 32:b * 64 + (part + 1) * 32, g * 128:(g + 1) * 128]
                              for b in range(4)]
                    rows += swap_blocks(blocks, lane)
                cols.append(jnp.concatenate(rows, axis=0))
            spec = jnp.dot(jnp.concatenate(cols, axis=1), w3[...], precision=HIGHEST, preferred_element_type=jnp.float32)
            sr, si = spec[:, :128], spec[:, 128:]

            @pl.when(c >= SLOTS)
            def _():
                wait_sent(2, "pz", send3, to)
            gr, gi = g_re[slot], g_im[slot]
            hat_re[c] = sr * gr - si * gi
            hat_im[c] = sr * gi + si * gr
            back = jnp.dot(jnp.concatenate([hat_re[c], hat_im[c]], axis=1), w4[...], precision=HIGHEST,
                           preferred_element_type=jnp.float32)
            for part in range(2):
                for g in range(2):
                    blocks = [back[(4 * g + k) * 32:(4 * g + k + 1) * 32, part * 128:(part + 1) * 128] for k in range(4)]
                    for b, block in enumerate(swap_blocks(blocks, lane)):
                        send3[to, b * 64 + part * 32:b * 64 + (part + 1) * 32, g * 128:(g + 1) * 128] = block
            exchange(2, "pz", send3, recv3, c)

        @pl.when((u >= 6) & (u < chunks + 6))
        def _():
            c = u - 6
            to, ring = lax.rem(c, SLOTS), lax.rem(c, RING)
            wait_received(2, recv3, c)

            @pl.when(c >= SLOTS)
            def _():
                wait_sent(3, "py", send4, to)
            back = jnp.dot(w5[...], recv3[ring], precision=HIGHEST, preferred_element_type=jnp.float32)
            for part in range(2):
                for g in range(2):
                    blocks = [back[part * 128 + y * 32:part * 128 + (y + 1) * 32, g * 128:(g + 1) * 128] for y in range(4)]
                    for k, block in enumerate(swap_blocks(blocks, lane)):
                        send4[to, pl.ds(part * 8 + 4 * g + k, 32, stride=16), :] = block
            exchange(3, "py", send4, recv4, c)

        @pl.when((lax.rem(u, 2) == 0) & (u >= 8))
        def _():
            c = u - 8
            f = lax.div(c, 2)
            for h in range(2):
                wait_received(3, recv4, c + h)
            out = last_dft(lambda h, rows: recv4[lax.rem(c + h, RING), rows, :], w6)
            phi_re[f] = out[:, :128]
            phi_im[f] = out[:, 128:]

        return carry

    lax.fori_loop(0, chunks + 6, step, 0)
    for c in range(chunks - 2, chunks):
        wait_received(3, recv4, c)
    for slot in range(SLOTS):
        wait_sent(0, "py", send1, slot)
        wait_sent(1, "pz", send2, slot)
        wait_sent(2, "pz", send3, slot)
        wait_sent(3, "py", send4, slot)


def write_out(phi_re, phi_im, hat_re, hat_im, recv4, m6, phi_re_out, phi_im_out, hat_re_out, hat_im_out, w6, last, sem):
    fields = phi_re.shape[0]
    weights = pltpu.make_async_copy(m6, w6, sem.at[6])
    copies = [pltpu.make_async_copy(src, dst, sem.at[i]) for i, (src, dst) in enumerate((
        (hat_re, hat_re_out), (hat_im, hat_im_out),
        (phi_re.at[pl.ds(0, fields - 1)], phi_re_out.at[pl.ds(0, fields - 1)]),
        (phi_im.at[pl.ds(0, fields - 1)], phi_im_out.at[pl.ds(0, fields - 1)])))]
    for cp in [weights] + copies:
        cp.start()
    weights.wait()
    out = last_dft(lambda h, rows: recv4[(2 * (fields - 1) + h) % RING, rows, :], w6)
    tail = [pltpu.make_async_copy(last.at[i], dst.at[fields - 1], sem.at[4 + i])
            for i, dst in enumerate((phi_re_out, phi_im_out))]
    for i, cp in enumerate(tail):
        last[i] = out[:, i * 128:(i + 1) * 128]
        cp.start()
    for cp in copies + tail:
        cp.wait()


def solution(mesh):
    npy, npz = mesh.shape["py"], mesh.shape["pz"]

    def local_solve(rho_re, rho_im, g_re, g_im):
        fields, n, ny, nz = rho_re.shape
        kx, ky = n // npy, n // npz
        fwd, inv = dft(n, -1), dft(n, 1)
        natural = np.arange(2 * n)
        x_blocks = order(n, (npy, 2, kx // 2), (2, 1, 0, 3))
        y_blocks = order(n, (npz, ky), (1, 0, 2))
        y_mixed = order(n, (npy, ny // 4, 4), (0, 3, 1, 2))
        pick = lambda m, r, c: jnp.asarray(m[np.ix_(r, c)].astype(np.float32))
        mats = (pick(fwd, x_blocks, natural), pick(fwd, y_blocks, y_mixed), pick(fwd.T, natural, natural),
                pick(inv.T, natural, natural), pick(inv, y_mixed, y_blocks), pick(inv.T, x_blocks, natural))
        lines = ny * nz
        half = lines // 2
        f32, any_space = jnp.float32, pl.BlockSpec(memory_space=pl.ANY)
        space = lambda v: v.transpose(0, 2, 3, 1).reshape(fields, lines, n)
        held = ((fields, lines, n),) * 2 + ((2 * fields, half, n),) * 2
        x_buf, y_buf = (lines, n), (2 * n, 2 * n)
        square, vmem = (2 * n, 2 * n), pl.BlockSpec(memory_space=pltpu.VMEM)
        *out, tail = pl.pallas_call(
            functools.partial(kernel, fields, npy, npz),
            out_shape=[pltpu.VMEM(s, f32) for s in held + ((RING,) + x_buf,)],
            in_specs=[any_space] * 10,
            out_specs=[vmem] * 5,
            scratch_shapes=[pltpu.VMEM((2, half, n), f32)] * 2 + [pltpu.VMEM(square, f32)] * 6 + [
                pltpu.VMEM((2, 2, lines, n), f32), pltpu.VMEM(y_buf, f32)] + [
                pltpu.VMEM((SLOTS,) + b, f32) for b in (x_buf, y_buf, y_buf, x_buf)] + [
                pltpu.VMEM((RING,) + b, f32) for b in (x_buf, y_buf, y_buf)] + [
                pltpu.SemaphoreType.DMA((8,)), pltpu.SemaphoreType.DMA((2, 2)),
                pltpu.SemaphoreType.DMA((4, SLOTS)), pltpu.SemaphoreType.DMA((4, RING)),
            ],
            compiler_params=pltpu.CompilerParams(collective_id=0, has_side_effects=True, vmem_limit_bytes=22 * 2**20),
        )(*[pltpu.with_memory_space_constraint(v, pltpu.HBM) for v in (
            space(rho_re), space(rho_im), g_re.reshape(2, half, n), g_im.reshape(2, half, n), *mats)])
        out = pl.pallas_call(
            write_out,
            out_shape=[jax.ShapeDtypeStruct(s, f32) for s in held],
            in_specs=[vmem] * 5 + [any_space], out_specs=[any_space] * 4,
            scratch_shapes=[pltpu.VMEM(square, f32), pltpu.VMEM((2, lines, n), f32), pltpu.SemaphoreType.DMA((7,))],
            compiler_params=pltpu.CompilerParams(vmem_limit_bytes=4 * 2**20),
        )(*[pltpu.with_memory_space_constraint(v, pltpu.VMEM) for v in (*out, tail)], mats[5])
        grid = lambda v: v.reshape(fields, ny, nz, n).transpose(0, 3, 1, 2)
        wave = lambda v: v.reshape(fields, kx, ky, n)
        return grid(out[0]), grid(out[1]), wave(out[2]), wave(out[3])

    space_layout = P("dp", None, "py", "pz")
    wave_layout = P("dp", "py", "pz", None)
    green_layout = P("py", "pz", None)
    return jax.shard_map(local_solve, mesh=mesh,
                         in_specs=(space_layout, space_layout, green_layout, green_layout),
                         out_specs=(space_layout, space_layout, wave_layout, wave_layout),
                         check_vma=False)
```
